64 devices in a mesh: dp: 4 (over x, y), tp: 16 (over z, core).
Axes of the slice: x: 2, y: 2, z: 8, core: 2. Of those that a mesh axis runs over, the one named last changes fastest.
The devices are a block of a 4x4x8 slice.
Arguments:
- x_in: bfloat16 [64, 4096], P('dp'), parts along dimension 0
- tok_pos: int32 [64], P('dp'), parts along dimension 0
- conv_state: bfloat16 [2, 64, 3, 4096], P(None, 'dp', None, 'tp'), parts along dimension 1
- lru_state: float32 [2, 64, 4096], P(None, 'dp', 'tp'), parts along dimension 1
- k_cache: bfloat16 [64, 2048, 256], P('dp'), parts along dimension 0
- v_cache: bfloat16 [64, 2048, 256], P('dp'), parts along dimension 0
- slot_pos: int32 [64, 2048], P('dp'), parts along dimension 0
- norm_scale: bfloat16 [3, 2, 4096], replicated
- rec_wx: bfloat16 [2, 4096, 4096], P(None, None, 'tp')
- rec_bx: bfloat16 [2, 4096], P(None, 'tp')
- rec_wy: bfloat16 [2, 4096, 4096], P(None, None, 'tp')
- rec_by: bfloat16 [2, 4096], P(None, 'tp')
- conv_w: bfloat16 [2, 4, 4096], P(None, None, 'tp')
- conv_b: bfloat16 [2, 4096], P(None, 'tp')
- gate_wa: bfloat16 [2, 16, 256, 256], P(None, 'tp')
- gate_ba: bfloat16 [2, 4096], P(None, 'tp')
- gate_wi: bfloat16 [2, 16, 256, 256], P(None, 'tp')
- gate_bi: bfloat16 [2, 4096], P(None, 'tp')
- a_param: float32 [2, 4096], P(None, 'tp')
- rec_wout: bfloat16 [2, 4096, 4096], P(None, 'tp')
- rec_bout: bfloat16 [2, 4096], replicated
- attn_wq: bfloat16 [4096, 4096], P(None, 'tp')
- attn_wk: bfloat16 [4096, 256], replicated
- attn_wv: bfloat16 [4096, 256], replicated
- attn_wo: bfloat16 [4096, 4096], P('tp')
- attn_bo: bfloat16 [4096], replicated
- mlp_w1: bfloat16 [3, 4096, 12288], P(None, None, 'tp')
- mlp_b1: bfloat16 [3, 12288], P(None, 'tp')
- mlp_w2: bfloat16 [3, 4096, 12288], P(None, None, 'tp')
- mlp_b2: bfloat16 [3, 12288], P(None, 'tp')
- mlp_wd: bfloat16 [3, 12288, 4096], P(None, 'tp')
- mlp_bd: bfloat16 [3, 4096], replicated
Outputs:
- output 1: bfloat16 [64, 4096], P('dp'), parts along dimension 0
- output 2: bfloat16 [2, 64, 3, 4096], P(None, 'dp', None, 'tp'), parts along dimension 1
- output 3: float32 [2, 64, 4096], P(None, 'dp', 'tp'), parts along dimension 1
- output 4: bfloat16 [64, 2048, 256], P('dp'), parts along dimension 0
- output 5: bfloat16 [64, 2048, 256], P('dp'), parts along dimension 0
- output 6: int32 [64, 2048], P('dp'), parts along dimension 0
There are 4 independent parts. The reference program is written for one: setup_inputs(seed, part) draws one part's arguments, and reference() takes and returns one part's arrays. A program takes and returns all parts, laid end to end along the dimension named above; an argument that names none is the same for every part.
All inputs are finite; a program needn't handle non-finite values.
Results may differ from the reference program's by a relative error of at most 0.02.
Values are sent between devices in bfloat16 or wider.
A program may use at most 768 MiB of HBM per device.

```python
import jax
import jax.numpy as jnp
from jax import lax

D = 4096
L = 4096
H = 16
F = 12288
HEAD = 256
WINDOW = 2048
BATCH = 16

ROPE_BASE = 10000.0
NORM_EPS = 1e-6


def draw_positions(key):
    key_kind, key_low, key_mid, key_high, key_old = jax.random.split(key, 5)
    pos_kind = jax.random.permutation(key_kind, jnp.arange(BATCH, dtype=jnp.int32) % 4)
    pos_low = jax.random.randint(key_low, (BATCH,), 1, 8, dtype=jnp.int32)
    pos_mid = jax.random.randint(key_mid, (BATCH,), 8, WINDOW, dtype=jnp.int32)
    pos_high = jax.random.randint(key_high, (BATCH,), WINDOW, 4 * WINDOW, dtype=jnp.int32)
    tok_pos = jnp.where(pos_kind == 0, 0, jnp.where(pos_kind == 1, pos_low, jnp.where(pos_kind == 2, pos_mid, pos_high)))
    old_len = jax.random.randint(key_old, (BATCH,), 0, 4 * WINDOW, dtype=jnp.int32)
    written = jnp.where(tok_pos > 0, tok_pos, old_len)
    slot_ids = jnp.arange(WINDOW, dtype=jnp.int32)
    behind = written[:, None] - 1 - slot_ids[None, :]
    slot_pos = jnp.where(behind >= 0, slot_ids[None, :] + WINDOW * (behind // WINDOW), -1)
    return tok_pos.astype(jnp.int32), slot_pos.astype(jnp.int32)


def normal_draw(key, shape, scale):
    return (jax.random.normal(key, shape, jnp.float32) * scale).astype(jnp.bfloat16)


def setup_inputs(seed: int = 0, part: int = 0) -> dict:
    root_key = jax.random.key(seed)
    part_root, shared_root = jax.random.split(root_key)
    part_keys = jax.random.split(jax.random.fold_in(part_root, part), 8)
    weight_keys = jax.random.split(shared_root, 32)
    tok_pos, slot_pos = draw_positions(part_keys[0])
    v_mean = jax.random.normal(part_keys[6], (BATCH, 1, HEAD), jnp.float32)
    v_noise = jax.random.normal(part_keys[5], (BATCH, WINDOW, HEAD), jnp.float32)
    a_root = jax.random.uniform(weight_keys[11], (2, L), jnp.float32, 0.9, 0.999)
    a_soft = -jnp.log(a_root) / 8.0
    block_width = L // H
    return {
        'x_in': normal_draw(part_keys[1], (BATCH, D), 1.0),
        'tok_pos': tok_pos,
        'conv_state': normal_draw(part_keys[2], (2, BATCH, 3, L), 1.0),
        'lru_state': jax.random.normal(part_keys[3], (2, BATCH, L), jnp.float32) * 0.35,
        'k_cache': normal_draw(part_keys[4], (BATCH, WINDOW, HEAD), 1.0),
        'v_cache': (v_mean + v_noise).astype(jnp.bfloat16),
        'slot_pos': slot_pos,
        'norm_scale': normal_draw(weight_keys[0], (3, 2, D), 0.3),
        'rec_wx': normal_draw(weight_keys[1], (2, D, L), D ** -0.5),
        'rec_bx': normal_draw(weight_keys[2], (2, L), 0.3),
        'rec_wy': normal_draw(weight_keys[3], (2, D, L), D ** -0.5),
        'rec_by': normal_draw(weight_keys[4], (2, L), 0.3),
        'conv_w': normal_draw(weight_keys[5], (2, 4, L), 0.5),
        'conv_b': normal_draw(weight_keys[6], (2, L), 0.3),
        'gate_wa': normal_draw(weight_keys[7], (2, H, block_width, block_width), 2.0 * block_width ** -0.5),
        'gate_ba': normal_draw(weight_keys[8], (2, L), 1.5),
        'gate_wi': normal_draw(weight_keys[9], (2, H, block_width, block_width), block_width ** -0.5),
        'gate_bi': normal_draw(weight_keys[10], (2, L), 0.5),
        'a_param': jnp.log(jnp.expm1(a_soft)),
        'rec_wout': normal_draw(weight_keys[12], (2, L, D), L ** -0.5),
        'rec_bout': normal_draw(weight_keys[13], (2, D), 0.2),
        'attn_wq': normal_draw(weight_keys[14], (D, H * HEAD), D ** -0.5),
        'attn_wk': normal_draw(weight_keys[15], (D, HEAD), D ** -0.5),
        'attn_wv': normal_draw(weight_keys[16], (D, HEAD), D ** -0.5),
        'attn_wo': normal_draw(weight_keys[17], (H * HEAD, D), (H * HEAD) ** -0.5),
        'attn_bo': normal_draw(weight_keys[18], (D,), 0.2),
        'mlp_w1': normal_draw(weight_keys[19], (3, D, F), D ** -0.5),
        'mlp_b1': normal_draw(weight_keys[20], (3, F), 0.3),
        'mlp_w2': normal_draw(weight_keys[21], (3, D, F), D ** -0.5),
        'mlp_b2': normal_draw(weight_keys[22], (3, F), 0.3),
        'mlp_wd': normal_draw(weight_keys[23], (3, F, D), F ** -0.5),
        'mlp_bd': normal_draw(weight_keys[24], (3, D), 0.2),
    }


def rms_norm(residual, scale):
    res_f = residual.astype(jnp.float32)
    mean_sq = jnp.mean(res_f * res_f, axis=-1, keepdims=True)
    return (res_f * lax.rsqrt(mean_sq + NORM_EPS) * (1.0 + scale.astype(jnp.float32))).astype(jnp.bfloat16)


def add_update(residual, update, out_bias):
    return (residual.astype(jnp.float32) + update.astype(jnp.bfloat16).astype(jnp.float32) + out_bias.astype(jnp.float32)).astype(jnp.bfloat16)


def rope_tables(tok_pos, head_dim):
    quarter = head_dim // 4
    inv_freq = ROPE_BASE ** (-jnp.arange(quarter, dtype=jnp.float32) / quarter)
    angles = tok_pos.astype(jnp.float32)[:, None] * inv_freq[None, :]
    return jnp.cos(angles), jnp.sin(angles)


def apply_rope(vectors, cosine, sine):
    quarter = vectors.shape[-1] // 4
    first = vectors[..., :quarter]
    second = vectors[..., quarter:2 * quarter]
    return jnp.concatenate([first * cosine - second * sine, second * cosine + first * sine, vectors[..., 2 * quarter:]], axis=-1)


def mlp_update(normed, w_up, b_up, w_lin, b_lin, w_down):
    gate_pre = jnp.dot(normed, w_up, preferred_element_type=jnp.float32) + b_up.astype(jnp.float32)
    lin_pre = jnp.dot(normed, w_lin, preferred_element_type=jnp.float32) + b_lin.astype(jnp.float32)
    hidden = (jax.nn.gelu(gate_pre, approximate=True) * lin_pre).astype(jnp.bfloat16)
    return jnp.dot(hidden, w_down, preferred_element_type=jnp.float32)


def recurrent_update(normed, tok_pos, conv_prev, lru_prev, rec_wx, rec_bx, rec_wy, rec_by, conv_w, conv_b, gate_wa, gate_ba, gate_wi, gate_bi, a_param, rec_wout):
    n_rows = normed.shape[0]
    n_blocks = gate_wa.shape[0]
    block_width = gate_wa.shape[1]
    x_branch = (jnp.dot(normed, rec_wx, preferred_element_type=jnp.float32) + rec_bx.astype(jnp.float32)).astype(jnp.bfloat16)
    y_branch = jax.nn.gelu(jnp.dot(normed, rec_wy, preferred_element_type=jnp.float32) + rec_by.astype(jnp.float32), approximate=True)
    tap_keep = tok_pos[:, None, None] >= jnp.arange(3, 0, -1, dtype=jnp.int32)[None, :, None]
    history = jnp.where(tap_keep, conv_prev.astype(jnp.float32), 0.0)
    tap_w = conv_w.astype(jnp.float32)
    conv_sum = conv_b.astype(jnp.float32) + tap_w[0] * x_branch.astype(jnp.float32) + jnp.sum(history * tap_w[:0:-1][None], axis=1)
    conv_x = conv_sum.astype(jnp.bfloat16)
    blocks = conv_x.reshape(n_rows, n_blocks, block_width).astype(jnp.float32)
    r_pre = jnp.einsum('bhi,hij->bhj', blocks, gate_wa.astype(jnp.float32)).reshape(n_rows, -1) + gate_ba.astype(jnp.float32)
    i_pre = jnp.einsum('bhi,hij->bhj', blocks, gate_wi.astype(jnp.float32)).reshape(n_rows, -1) + gate_bi.astype(jnp.float32)
    log_a = -8.0 * jax.nn.sigmoid(r_pre) * jax.nn.softplus(a_param)
    decay_gate = jnp.exp(log_a)
    in_scale = jnp.sqrt(1.0 - decay_gate * decay_gate)
    is_reset = (tok_pos == 0)[:, None]
    decay_gate = jnp.where(is_reset, 0.0, decay_gate)
    in_scale = jnp.where(is_reset, 1.0, in_scale)
    lru_new = decay_gate * lru_prev + in_scale * jax.nn.sigmoid(i_pre) * conv_x.astype(jnp.float32)
    gated_h = (lru_new * y_branch).astype(jnp.bfloat16)
    update = jnp.dot(gated_h, rec_wout, preferred_element_type=jnp.float32)
    conv_new = jnp.concatenate([conv_prev[:, 1:], x_branch[:, None, :]], axis=1)
    return update, conv_new, lru_new


def attention_update(normed, tok_pos, k_cache, v_cache, slot_pos, attn_wq, attn_wk, attn_wv, attn_wo):
    n_rows = normed.shape[0]
    head_dim = attn_wk.shape[1]
    window = k_cache.shape[1]
    cosine, sine = rope_tables(tok_pos, head_dim)
    q_heads = jnp.dot(normed, attn_wq, preferred_element_type=jnp.float32).reshape(n_rows, -1, head_dim)
    q_heads = apply_rope(q_heads, cosine[:, None, :], sine[:, None, :]).astype(jnp.bfloat16)
    k_new = apply_rope(jnp.dot(normed, attn_wk, preferred_element_type=jnp.float32), cosine, sine).astype(jnp.bfloat16)
    v_new = jnp.dot(normed, attn_wv, preferred_element_type=jnp.float32).astype(jnp.bfloat16)
    target = jnp.arange(window, dtype=jnp.int32)[None, :] == (tok_pos % window)[:, None]
    k_next = jnp.where(target[:, :, None], k_new[:, None, :], k_cache)
    v_next = jnp.where(target[:, :, None], v_new[:, None, :], v_cache)
    slot_next = jnp.where(target, tok_pos[:, None], slot_pos)
    slot_age = tok_pos[:, None] - slot_next
    slot_valid = (slot_next >= 0) & (slot_age >= 0) & (slot_age < window)

    def attend_row(row_args):
        q_row, k_row, v_row, valid_row = row_args
        scores = jnp.einsum('hd,sd->hs', q_row.astype(jnp.float32), k_row.astype(jnp.float32)) * (head_dim ** -0.5)
        scores = jnp.where(valid_row[None, :], scores, -jnp.inf)
        probs_bf = jax.nn.softmax(scores, axis=-1).astype(jnp.bfloat16)
        return jnp.einsum('hs,sd->hd', probs_bf.astype(jnp.float32), v_row.astype(jnp.float32)).astype(jnp.bfloat16)

    heads_out = lax.map(attend_row, (q_heads, k_next, v_next, slot_valid))
    update = jnp.dot(heads_out.reshape(n_rows, -1), attn_wo, preferred_element_type=jnp.float32)
    return update, k_next, v_next, slot_next


def reference(x_in, tok_pos, conv_state, lru_state, k_cache, v_cache, slot_pos, norm_scale, rec_wx, rec_bx, rec_wy, rec_by, conv_w, conv_b, gate_wa, gate_ba, gate_wi, gate_bi, a_param, rec_wout, rec_bout, attn_wq, attn_wk, attn_wv, attn_wo, attn_bo, mlp_w1, mlp_b1, mlp_w2, mlp_b2, mlp_wd, mlp_bd):
    residual = x_in
    conv_list = []
    lru_list = []
    for layer_idx in range(3):
        normed = rms_norm(residual, norm_scale[layer_idx, 0])
        if layer_idx < 2:
            update, conv_new, lru_new = recurrent_update(normed, tok_pos, conv_state[layer_idx], lru_state[layer_idx], rec_wx[layer_idx], rec_bx[layer_idx], rec_wy[layer_idx], rec_by[layer_idx], conv_w[layer_idx], conv_b[layer_idx], gate_wa[layer_idx], gate_ba[layer_idx], gate_wi[layer_idx], gate_bi[layer_idx], a_param[layer_idx], rec_wout[layer_idx])
            conv_list.append(conv_new)
            lru_list.append(lru_new)
            out_bias = rec_bout[layer_idx]
        else:
            update, k_next, v_next, slot_next = attention_update(normed, tok_pos, k_cache, v_cache, slot_pos, attn_wq, attn_wk, attn_wv, attn_wo)
            out_bias = attn_bo
        residual = add_update(residual, update, out_bias)
        normed = rms_norm(residual, norm_scale[layer_idx, 1])
        update = mlp_update(normed, mlp_w1[layer_idx], mlp_b1[layer_idx], mlp_w2[layer_idx], mlp_b2[layer_idx], mlp_wd[layer_idx])
        residual = add_update(residual, update, mlp_bd[layer_idx])
    return (residual, jnp.stack(conv_list), jnp.stack(lru_list), k_next, v_next, slot_next)
```

```python
import functools

import jax
import jax.numpy as jnp
import numpy as np
from jax import lax
from jax.experimental import pallas as pl
from jax.experimental.pallas import tpu as pltpu
from jax.sharding import PartitionSpec as P

ROPE_BASE = 10000.0
NORM_EPS = 1e-6
F32 = jnp.float32
BF16 = jnp.bfloat16
MESH_ID = pl.DeviceIdType.MESH
VMEM_LIMIT = 67043328
ANY = pl.BlockSpec(memory_space=pl.ANY)
SMEM = pl.BlockSpec(memory_space=pltpu.SMEM)
VMEM = pl.BlockSpec(memory_space=pltpu.VMEM)


def gelu(x):
    return jax.nn.gelu(x, approximate=True)


def softplus(x):
    return jnp.maximum(x, 0.0) + jnp.log1p(jnp.exp(-jnp.abs(x)))


def lane_positions(pos_ref, width):
    rows = pos_ref.shape[0]
    row_ids = lax.broadcasted_iota(jnp.int32, (rows, width), 0)
    out = jnp.zeros((rows, width), jnp.int32)
    for b in range(rows):
        out = jnp.where(row_ids == b, pos_ref[b], out)
    return out


class Group:
    def __init__(self, n, sendb, rsb, res, ssem, rsem):
        self.n, self.sendb, self.rsb, self.res, self.ssem, self.rsem = n, sendb, rsb, res, ssem, rsem
        self.me = lax.axis_index("tp")
        self.chunk = res.shape[2]
        self.order = sorted(range(1, n), key=lambda k: -min(k, n - k))
        self.rs_open, self.ag_open = [], []

    def peer(self, k):
        return lax.rem(self.me + k, self.n)

    def greet(self):
        barrier = pltpu.get_barrier_semaphore()
        for k in range(1, self.n):
            pl.semaphore_signal(barrier, inc=1, device_id={"tp": self.peer(k)}, device_id_type=MESH_ID)

    def wait_greet(self):
        pl.semaphore_wait(pltpu.get_barrier_semaphore(), self.n - 1)

    def cols(self, d):
        return pl.ds(pl.multiple_of(d * self.chunk, self.chunk), self.chunk)

    def norm(self, scale_ref, layer, which, nb):
        chunk = self.chunk
        total = None
        for c in range(self.n):
            x = self.res[c].astype(F32)
            total = x * x if total is None else total + x * x
        inv = lax.rsqrt(jnp.sum(total, axis=1, keepdims=True) / (self.n * chunk) + NORM_EPS)
        for c in range(self.n):
            lanes = slice(c * chunk, (c + 1) * chunk)
            scale = 1.0 + scale_ref[layer, which:which + 1, lanes].astype(F32)
            nb[:, lanes] = (self.res[c].astype(F32) * inv * scale).astype(BF16)

    def scatter(self, h, w_ref):
        for copy in self.rs_open:
            copy.wait_send()
        self.rs_open = []
        late = None
        for k in self.order + [0]:
            dst = self.peer(k) if k else self.me
            part = jnp.dot(h, w_ref[:, self.cols(dst)], preferred_element_type=F32)
            if late is not None:
                late.start()
            if k:
                self.sendb[k] = part.astype(BF16)
                late = pltpu.make_async_remote_copy(
                    src_ref=self.sendb.at[k], dst_ref=self.rsb.at[k], send_sem=self.ssem.at[0, k], recv_sem=self.rsem.at[0, k],
                    device_id={"tp": dst}, device_id_type=MESH_ID)
                self.rs_open.append(late)
            else:
                late = None
        return part

    def finish(self, own, bias_row):
        for copy in self.rs_open:
            copy.wait_recv()
        for k in self.order:
            own = own + self.rsb[k].astype(F32)
        update = own.astype(BF16).astype(F32)
        fresh = (self.res[self.me].astype(F32) + update + bias_row.astype(F32)).astype(BF16)
        for copy in self.ag_open:
            copy.wait_send()
        self.ag_open = []
        self.res[self.me] = fresh
        for k in self.order:
            copy = pltpu.make_async_remote_copy(
                src_ref=self.res.at[self.me], dst_ref=self.res.at[self.me], send_sem=self.ssem.at[1, k], recv_sem=self.rsem.at[1, k],
                device_id={"tp": self.peer(k)}, device_id_type=MESH_ID)
            copy.start()
            self.ag_open.append(copy)
        for copy in self.ag_open:
            copy.wait_recv()
        return fresh

    def close(self):
        for copy in self.rs_open + self.ag_open:
            copy.wait_send()


def mlp(group, layer, nb, hb, w1, w2, wd, b1, b2, bd, waits):
    step = 256
    waits[0].wait()
    waits[1].wait()
    n = nb[...]
    for j in range(hb.shape[1] // step):
        lanes = slice(j * step, (j + 1) * step)
        gate = jnp.dot(n, w1[:, lanes], preferred_element_type=F32) + b1[layer:layer + 1, lanes].astype(F32)
        lin = jnp.dot(n, w2[:, lanes], preferred_element_type=F32) + b2[layer:layer + 1, lanes].astype(F32)
        hb[:, lanes] = (gelu(gate) * lin).astype(BF16)
    waits[2].wait()
    own = group.scatter(hb[...], wd)
    return group.finish(own, bd[layer:layer + 1, group.cols(group.me)])


FIRST_SMALL = ("x", "nscale", "conv", "lru", "bx", "by", "cw", "cb", "ba", "bi", "ap", "wa", "wi", "bout", "b1", "b2", "bd", "invf")
FIRST_BIG = ("wx", "wy", "wout", "w1", "w2", "wd", "wq", "wk", "wv")


def first_kernel(n, layers, pos_ref, *refs):
    names = FIRST_SMALL + FIRST_BIG
    hbm = dict(zip(names, refs))
    refs = refs[len(names):]
    xown_ref, q_ref, kn_ref, vn_ref, convo_ref, lruo_ref = refs[:6]
    refs = refs[6:]
    small = dict(zip(FIRST_SMALL, refs))
    refs = refs[len(FIRST_SMALL):]
    wxs, wys, wos, w1s, w2s, wds, qkv, nb, hb, sendb, rsb, res, ssem, rsem, lsem, bsem = refs

    group = Group(n, sendb, rsb, res, ssem, rsem)
    group.greet()

    def start(src, dst, sem, priority=0):
        copy = pltpu.make_async_copy(src, dst, sem)
        copy.start(priority=priority)
        return copy

    loads = {name: start(hbm[name], small[name], lsem.at[i]) for i, name in enumerate(FIRST_SMALL)}
    big = {}
    count = 0
    for l in range(layers):
        for name, dst in (("wx", wxs), ("wy", wys), ("wout", wos), ("w1", w1s), ("w2", w2s), ("wd", wds)):
            big[name, l] = start(hbm[name].at[l], dst.at[l], bsem.at[count], 1)
            count += 1
    for i, name in enumerate(("wq", "wk", "wv")):
        big[name] = start(hbm[name], qkv.at[i], bsem.at[count], 1)
        count += 1

    for copy in loads.values():
        copy.wait()
    chunk = res.shape[2]
    for c in range(n):
        res[c] = small["x"][:, c * chunk:(c + 1) * chunk]
    pos = lane_positions(pos_ref, chunk)

    def row(name, l):
        return small[name][l:l + 1, :].astype(F32)

    for l in range(layers):
        group.norm(small["nscale"], l, 0, nb)
        big["wx", l].wait()
        xb = (jnp.dot(nb[...], wxs[l], preferred_element_type=F32) + row("bx", l)).astype(BF16)
        big["wy", l].wait()
        y = gelu(jnp.dot(nb[...], wys[l], preferred_element_type=F32) + row("by", l))
        taps = [small["cw"][l, j:j + 1, :].astype(F32) for j in range(4)]
        old = small["conv"][l].astype(F32)
        hist = None
        for j in range(3):
            term = jnp.where(pos >= 3 - j, old[:, j, :], 0.0) * taps[3 - j]
            hist = term if hist is None else hist + term
        xc = (row("cb", l) + taps[0] * xb.astype(F32) + hist).astype(BF16)
        r_pre = jnp.dot(xc, small["wa"][l, 0], preferred_element_type=F32) + row("ba", l)
        i_pre = jnp.dot(xc, small["wi"][l, 0], preferred_element_type=F32) + row("bi", l)
        decay = jnp.exp(-8.0 * jax.nn.sigmoid(r_pre) * softplus(small["ap"][l:l + 1, :]))
        in_scale = jnp.sqrt(1.0 - decay * decay)
        decay = jnp.where(pos == 0, 0.0, decay)
        in_scale = jnp.where(pos == 0, 1.0, in_scale)
        h = decay * small["lru"][l] + in_scale * jax.nn.sigmoid(i_pre) * xc.astype(F32)
        big["wout", l].wait()
        if l == 0:
            group.wait_greet()
        own = group.scatter((h * y).astype(BF16), wos.at[l])
        lruo_ref[l] = h
        convo_ref[l] = jnp.stack([old[:, 1, :], old[:, 2, :], xb.astype(F32)], axis=1).astype(BF16)
        group.finish(own, small["bout"][l:l + 1, group.cols(group.me)])

        group.norm(small["nscale"], l, 1, nb)
        fresh = mlp(group, l, nb, hb, w1s.at[l], w2s.at[l], wds.at[l], small["b1"], small["b2"], small["bd"],
                    (big["w1", l], big["w2", l], big["wd", l]))

    xown_ref[...] = fresh
    group.norm(small["nscale"], layers, 0, nb)
    half = small["invf"].shape[1]
    angles = pos[:, :half].astype(F32) * small["invf"][...]
    cosine, sine = jnp.cos(angles), jnp.sin(angles)
    lane = lax.broadcasted_iota(jnp.int32, sine.shape, 1)
    sine = jnp.where(lane < half // 2, -sine, sine)

    def rope(v):
        turned = v[:, :half]
        return jnp.concatenate([turned * cosine + pltpu.roll(turned, half // 2, 1) * sine, v[:, half:]], axis=1)

    big["wq"].wait()
    q_ref[...] = rope(jnp.dot(nb[...], qkv[0], preferred_element_type=F32)).astype(BF16)
    big["wk"].wait()
    kn_ref[...] = rope(jnp.dot(nb[...], qkv[1], preferred_element_type=F32)).astype(BF16)
    big["wv"].wait()
    vn_ref[...] = jnp.dot(nb[...], qkv[2], preferred_element_type=F32).astype(BF16)
    group.close()


def attend_kernel(pos_ref, q_ref, kn_ref, vn_ref, conv_ref, lru_ref, slot_ref, k_hbm, v_hbm,
                  o_ref, convo_ref, lruo_ref, sloto_ref, ko_hbm, vo_hbm, kb, vb, bias, sems):
    rows, window, dim = k_hbm.shape
    loads, stores = [], []
    for b in range(rows):
        pair = []
        for i, (src, dst) in enumerate(((k_hbm, kb), (v_hbm, vb))):
            copy = pltpu.make_async_copy(src.at[b], dst.at[b], sems.at[0, i, b])
            copy.start()
            pair.append(copy)
        loads.append(pair)
    convo_ref[...] = conv_ref[...]
    lruo_ref[...] = lru_ref[...]
    pos = lane_positions(pos_ref, window)
    lane = lax.broadcasted_iota(jnp.int32, pos.shape, 1)
    slots = jnp.where(lane == lax.rem(pos, window), pos, slot_ref[...])
    sloto_ref[...] = slots
    age = pos - slots
    bias[...] = jnp.where((slots >= 0) & (age >= 0) & (age < window), 0.0, -jnp.inf)
    pack = 16
    sub = lax.broadcasted_iota(jnp.int32, (pack, dim), 0)
    for b in range(rows):
        slot = lax.rem(pos_ref[b], window)
        base = pl.multiple_of(slot // pack * pack, pack)
        for i, (buf, new) in enumerate(((kb, kn_ref), (vb, vn_ref))):
            loads[b][i].wait()
            tile = buf[b, pl.ds(base, pack), :]
            buf[b, pl.ds(base, pack), :] = jnp.where(sub == slot - base, new[b:b + 1, :].astype(F32), tile.astype(F32)).astype(BF16)
        scores = lax.dot_general(q_ref[b:b + 1, :], kb[b], (((1,), (1,)), ((), ())), preferred_element_type=F32)
        for i, (buf, dst) in enumerate(((kb, ko_hbm), (vb, vo_hbm))):
            copy = pltpu.make_async_copy(buf.at[b], dst.at[b], sems.at[1, i, b])
            copy.start()
            stores.append(copy)
        scores = scores * (dim ** -0.5) + bias[b:b + 1, :]
        weight = jnp.exp(scores - jnp.max(scores, axis=1, keepdims=True))
        probs = (weight / jnp.sum(weight, axis=1, keepdims=True)).astype(BF16)
        o_ref[b:b + 1, :] = jnp.dot(probs, vb[b], preferred_element_type=F32).astype(BF16)
    for copy in stores:
        copy.wait()


LAST_SMALL = ("o", "xown", "nscale", "bo", "b1", "b2", "bd")
LAST_BIG = ("wo", "w1", "w2", "wd")


def last_kernel(n, layer, *refs):
    names = LAST_SMALL + LAST_BIG
    hbm = dict(zip(names, refs))
    refs = refs[len(names):]
    x_ref = refs[0]
    refs = refs[1:]
    small = dict(zip(LAST_SMALL, refs))
    refs = refs[len(LAST_SMALL):]
    wos, w1s, w2s, wds, nb, hb, sendb, rsb, res, ssem, rsem, lsem, bsem = refs
    group = Group(n, sendb, rsb, res, ssem, rsem)
    group.greet()

    def start(src, dst, sem, priority=0):
        copy = pltpu.make_async_copy(src, dst, sem)
        copy.start(priority=priority)
        return copy

    loads = [start(hbm[name], small[name], lsem.at[i]) for i, name in enumerate(LAST_SMALL)]
    big = [start(hbm["wo"], wos, bsem.at[0], 1)]
    for i, (name, dst) in enumerate((("w1", w1s), ("w2", w2s), ("wd", wds))):
        big.append(start(hbm[name].at[layer], dst, bsem.at[i + 1], 1))
    for copy in loads:
        copy.wait()
    res[group.me] = small["xown"][...]
    big[0].wait()
    group.wait_greet()
    own = group.scatter(small["o"][...], wos)
    group.finish(own, small["bo"][:, group.cols(group.me)])
    group.norm(small["nscale"], layer, 1, nb)
    mlp(group, layer, nb, hb, w1s, w2s, wds, small["b1"], small["b2"], small["bd"], big[1:])
    chunk = res.shape[2]
    for c in range(n):
        x_ref[:, c * chunk:(c + 1) * chunk] = res[c]
    group.close()


def io_specs():
    in_specs = (P('dp', None), P('dp'), P(None, 'dp', None, 'tp'), P(None, 'dp', 'tp'), P('dp', None, None), P('dp', None, None), P('dp', None),
                P(), P(None, None, 'tp'), P(None, 'tp'), P(None, None, 'tp'), P(None, 'tp'), P(None, None, 'tp'), P(None, 'tp'),
                P(None, 'tp', None, None), P(None, 'tp'), P(None, 'tp', None, None), P(None, 'tp'), P(None, 'tp'), P(None, 'tp', None), P(),
                P(None, 'tp'), P(), P(), P('tp', None), P(),
                P(None, None, 'tp'), P(None, 'tp'), P(None, None, 'tp'), P(None, 'tp'), P(None, 'tp', None), P())
    out_specs = (P('dp', None), P(None, 'dp', None, 'tp'), P(None, 'dp', 'tp'), P('dp', None, None), P('dp', None, None), P('dp', None))
    return in_specs, out_specs


def vmem_like(array):
    return pltpu.VMEM(array.shape, array.dtype)


def solution(mesh):
    in_specs, out_specs = io_specs()
    n = mesh.shape["tp"]

    def local_step(x_in, tok_pos, conv_state, lru_state, k_cache, v_cache, slot_pos, norm_scale, rec_wx, rec_bx, rec_wy, rec_by, conv_w, conv_b, gate_wa, gate_ba, gate_wi, gate_bi, a_param, rec_wout, rec_bout, attn_wq, attn_wk, attn_wv, attn_wo, attn_bo, mlp_w1, mlp_b1, mlp_w2, mlp_b2, mlp_wd, mlp_bd):
        rows, width = x_in.shape
        layers, _, own = rec_wx.shape
        hidden = mlp_w1.shape[2]
        head_dim = attn_wk.shape[1]
        window = k_cache.shape[1]
        chunk = width // n
        quarter = head_dim // 4
        freq = np.float64(ROPE_BASE) ** (-np.arange(quarter, dtype=np.float64) / quarter)
        invf = jnp.asarray(np.concatenate([freq, freq]).astype(np.float32)[None, :])
        exchange = [pltpu.VMEM((n, rows, chunk), BF16), pltpu.VMEM((n, rows, chunk), BF16), pltpu.VMEM((n, rows, chunk), BF16),
                    pltpu.SemaphoreType.DMA((2, n)), pltpu.SemaphoreType.DMA((2, n))]
        small = (x_in, norm_scale, conv_state, lru_state, rec_bx, rec_by, conv_w, conv_b, gate_ba, gate_bi, a_param, gate_wa, gate_wi,
                 rec_bout, mlp_b1, mlp_b2, mlp_bd, invf)
        big = (rec_wx, rec_wy, rec_wout, mlp_w1, mlp_w2, mlp_wd, attn_wq, attn_wk, attn_wv)
        row_out = jax.ShapeDtypeStruct((rows, chunk), BF16)
        head_out = jax.ShapeDtypeStruct((rows, head_dim), BF16)
        x_own, q, k_new, v_new, conv_new, lru_new = pl.pallas_call(
            functools.partial(first_kernel, n, layers),
            out_shape=(row_out, head_out, head_out, head_out,
                       jax.ShapeDtypeStruct(conv_state.shape, BF16), jax.ShapeDtypeStruct(lru_state.shape, F32)),
            in_specs=[SMEM] + [ANY] * (len(small) + len(big)),
            out_specs=(VMEM,) * 6,
            scratch_shapes=[vmem_like(a) for a in small] + [
                vmem_like(rec_wx), vmem_like(rec_wy), vmem_like(rec_wout),
                pltpu.VMEM((layers,) + mlp_w1.shape[1:], BF16), pltpu.VMEM((layers,) + mlp_w2.shape[1:], BF16),
                pltpu.VMEM((layers,) + mlp_wd.shape[1:], BF16), pltpu.VMEM((3,) + attn_wk.shape, BF16),
                pltpu.VMEM((rows, width), BF16), pltpu.VMEM((rows, hidden), BF16)] + exchange + [
                pltpu.SemaphoreType.DMA((len(small),)), pltpu.SemaphoreType.DMA((6 * layers + 3,))],
            compiler_params=pltpu.CompilerParams(collective_id=0, has_side_effects=True, vmem_limit_bytes=VMEM_LIMIT),
            name="recurrent_layers",
        )(tok_pos, *small, *big)

        heads, conv_out, lru_out, slot_out, k_out, v_out = pl.pallas_call(
            attend_kernel,
            out_shape=(head_out, jax.ShapeDtypeStruct(conv_state.shape, BF16), jax.ShapeDtypeStruct(lru_state.shape, F32),
                       jax.ShapeDtypeStruct(slot_pos.shape, jnp.int32), jax.ShapeDtypeStruct(k_cache.shape, BF16),
                       jax.ShapeDtypeStruct(v_cache.shape, BF16)),
            in_specs=[SMEM] + [VMEM] * 6 + [ANY] * 2,
            out_specs=(VMEM,) * 4 + (ANY,) * 2,
            scratch_shapes=[vmem_like(k_cache), vmem_like(v_cache), pltpu.VMEM((rows, window), F32), pltpu.SemaphoreType.DMA((2, 2, rows))],
            compiler_params=pltpu.CompilerParams(vmem_limit_bytes=VMEM_LIMIT),
            name="attend",
        )(tok_pos, q, k_new, v_new, conv_new, lru_new, slot_pos, k_cache, v_cache)

        tail = (heads, x_own, norm_scale, attn_bo[None, :], mlp_b1, mlp_b2, mlp_bd)
        x_out = pl.pallas_call(
            functools.partial(last_kernel, n, layers),
            out_shape=jax.ShapeDtypeStruct((rows, width), BF16),
            in_specs=[ANY] * (len(tail) + 4),
            out_specs=VMEM,
            scratch_shapes=[vmem_like(a) for a in tail] + [
                vmem_like(attn_wo), pltpu.VMEM(mlp_w1.shape[1:], BF16), pltpu.VMEM(mlp_w2.shape[1:], BF16), pltpu.VMEM(mlp_wd.shape[1:], BF16),
                pltpu.VMEM((rows, width), BF16), pltpu.VMEM((rows, hidden), BF16)] + exchange + [
                pltpu.SemaphoreType.DMA((len(tail),)), pltpu.SemaphoreType.DMA((4,))],
            compiler_params=pltpu.CompilerParams(collective_id=1, has_side_effects=True, vmem_limit_bytes=VMEM_LIMIT),
            name="last_mlp",
        )(*tail, attn_wo, mlp_w1, mlp_w2, mlp_wd)
        return (x_out, conv_out, lru_out, k_out, v_out, slot_out)

    return jax.shard_map(local_step, mesh=mesh, in_specs=in_specs, out_specs=out_specs, check_vma=False)
```
